32 devices in a mesh: dp: 4 (over x, y), tp: 8 (over z, core).
Axes of the slice: x: 2, y: 2, z: 4, core: 2. Of those that a mesh axis runs over, the one named last changes fastest.
Arguments:
- x: bfloat16 [5120, 7168], P(('dp', 'tp')), parts along dimension 0
- w_gate: bfloat16 [7168, 20480], P(None, 'tp')
- w_up: bfloat16 [7168, 20480], P(None, 'tp')
- w_down: bfloat16 [20480, 7168], P('tp')
Outputs:
- output: bfloat16 [5120, 7168], P(('dp', 'tp')), parts along dimension 0
There are 4 independent parts. The reference program is written for one: setup_inputs(seed, part) draws one part's arguments, and reference() takes and returns one part's arrays. A program takes and returns all parts, laid end to end along the dimension named above; an argument that names none is the same for every part.
All inputs are finite; a program needn't handle non-finite values.
Results may differ from the reference program's by a relative error of at most 0.016.
Values are sent between devices in bfloat16 or wider.
A program may use at most 2 GiB of HBM per device.

```python
import jax
import jax.numpy as jnp

ROWS = 1280
D = 7168
FF = 20480


def setup_inputs(seed: int = 0, part: int = 0) -> dict:
    kx, kg, ku, kd = jax.random.split(jax.random.key(seed), 4)
    drawn = {
        "x": jax.random.normal(jax.random.fold_in(kx, part), (ROWS, D), jnp.float32),
        "w_gate": jax.random.normal(kg, (D, FF), jnp.float32) * D**-0.5,
        "w_up": jax.random.normal(ku, (D, FF), jnp.float32) * D**-0.5,
        "w_down": jax.random.normal(kd, (FF, D), jnp.float32) * FF**-0.5,
    }
    return {k: v.astype(jnp.bfloat16) for k, v in drawn.items()}


def reference(x, w_gate, w_up, w_down):
    gate = jnp.dot(x, w_gate, preferred_element_type=jnp.float32)
    up = jnp.dot(x, w_up, preferred_element_type=jnp.float32)
    hidden = (jax.nn.silu(gate) * up).astype(jnp.bfloat16)
    return jnp.dot(hidden, w_down, preferred_element_type=jnp.float32).astype(jnp.bfloat16)
```

```python
import jax
import jax.numpy as jnp
from jax import lax
from jax.experimental import pallas as pl
from jax.experimental.pallas import tpu as pltpu
from jax.sharding import PartitionSpec as P

MESH = pl.DeviceIdType.MESH
F32, BF16 = jnp.float32, jnp.bfloat16

D = 7168
F = 2560
R = 160
NP, RP = 5, 32
KH = D // 2
GW, NG = 256, F // 256
DW, ND = 512, D // 512
TOT = 2 * NG + ND
NS = 4
PS = 4
LAG = 3


def kernel(x_ref, wg_ref, wu_ref, wd_ref, y_ref, xg, xb, ring, hid, acc, stash, pst, pt, rs,
           wsem, xsem, ag_recv, agp_recv, fwd_send, out_send, d2d_send,
           pst_send, pt_recv, rs_send, rs_recv, ysem):
    tp = lax.axis_index("tp")
    z, c = tp // 2, tp % 2
    mir = z // 2
    mid = (z * (3 - z)) // 2
    is_mid, is_end = mid == 1, mid == 0
    din = 1 - 2 * mir
    partner = {"tp": 2 * z + (1 - c)}
    inward = {"tp": 2 * (z + din) + c}
    outward = {"tp": 2 * (z - din * mid) + c}

    def real(bb):
        return bb + mir * (3 - 2 * bb)

    def block(s):
        m = ((s + 1) % 3) * (1 - s // 3) + 3 * (s // 3)
        return mid * m + (1 - mid) * s

    barrier = pltpu.get_barrier_semaphore()
    pl.semaphore_signal(barrier, inc=1, device_id=partner, device_id_type=MESH)
    pl.semaphore_signal(barrier, inc=1, device_id=inward, device_id_type=MESH)

    @pl.when(is_mid)
    def _():
        pl.semaphore_signal(barrier, inc=1, device_id=outward, device_id_type=MESH)

    def gu_copy(ref, i, kh, slot, h):
        return pltpu.make_async_copy(
            ref.at[pl.ds(pl.multiple_of(kh * KH, KH), KH), pl.ds(pl.multiple_of(i * GW, GW), GW)],
            ring.at[slot, :, pl.ds(h * GW, GW)], wsem.at[slot, h])

    def d_copy(j, slot):
        return pltpu.make_async_copy(
            wd_ref.at[:, pl.ds(pl.multiple_of(j * DW, DW), DW)],
            ring.at[slot, pl.ds(0, F)], wsem.at[slot, 0])

    def fetch(g):
        q, slot = lax.rem(g, TOT), lax.rem(g, NS)

        @pl.when((g < 4 * TOT) & (q < 2 * NG))
        def _():
            gu_copy(wg_ref, q // 2, q % 2, slot, 0).start()
            gu_copy(wu_ref, q // 2, q % 2, slot, 1).start()

        @pl.when((g < 4 * TOT) & (q >= 2 * NG))
        def _():
            d_copy(q - 2 * NG, slot).start()

    for k in range(NS - 1):
        fetch(jnp.int32(k))

    def rows(p):
        return pl.ds(pl.multiple_of(p * RP, RP), RP)

    def send_x(src, b, p, sem, recv, dev):
        return pltpu.make_async_remote_copy(
            src_ref=src.at[rows(p)], dst_ref=xg.at[b, c, rows(p)], send_sem=sem.at[b, p],
            recv_sem=recv.at[b, p], device_id=dev, device_id_type=MESH)

    def own_x(p, kind):
        if kind == 0:
            return send_x(x_ref, z, p, d2d_send, agp_recv, partner)
        if kind == 1:
            return send_x(x_ref, z, p, fwd_send, ag_recv, inward)
        return send_x(x_ref, z, p, out_send, ag_recv, outward)

    def arrived(b, p):
        send_x(xg.at[b, c], b, p, fwd_send, ag_recv, partner).wait_recv()

    def forward(b, p, dev):
        return send_x(xg.at[b, c], b, p, fwd_send, ag_recv, dev)

    def share(b, p):
        return send_x(xg.at[b, c], b, p, d2d_send, agp_recv, partner)

    def relay(s, p):
        @pl.when(is_end & (s < 3))
        def _():
            b = real(s + 1)
            arrived(b, p)
            share(b, p).start()

        @pl.when(is_mid & (s == 0))
        def _():
            b0, b2 = real(0), real(2)
            arrived(b2, p)
            forward(b2, p, outward).start()
            share(b2, p).start()
            arrived(b0, p)
            forward(b0, p, inward).start()
            share(b0, p).start()

        @pl.when(is_mid & (s == 1))
        def _():
            b3 = real(3)
            arrived(b3, p)
            forward(b3, p, outward).start()
            share(b3, p).start()

    def x_load_own(b):
        return pltpu.make_async_copy(xg.at[b, c], xb.at[pl.ds(0, R)], xsem.at[0])

    def x_load_partner(b):
        return pltpu.make_async_copy(xg.at[b, 1 - c], xb.at[pl.ds(R, R)], xsem.at[1])

    def wait_partner_x(b):
        @pl.loop(0, NP)
        def _(p):
            pltpu.make_async_remote_copy(
                src_ref=xg.at[b, 1 - c, rows(p)], dst_ref=xg.at[b, 1 - c, rows(p)],
                send_sem=d2d_send.at[b, p], recv_sem=agp_recv.at[b, p],
                device_id=partner, device_id_type=MESH).wait_recv()

    def send_pt(s, j):
        return pltpu.make_async_remote_copy(
            src_ref=pst.at[j % PS], dst_ref=pt.at[s % 2, j], send_sem=pst_send.at[j % PS],
            recv_sem=pt_recv.at[s % 2, j], device_id=partner, device_id_type=MESH)

    def send_rs(slot, there, j, dev):
        return pltpu.make_async_remote_copy(
            src_ref=rs.at[slot, j], dst_ref=rs.at[there, j], send_sem=rs_send.at[slot, j],
            recv_sem=rs_recv.at[there, j], device_id=dev, device_id_type=MESH)

    def rs_arrived(slot, j):
        send_rs(0, slot, j, inward).wait_recv()

    def fold(s, k):
        send_pt(s, k).wait_recv()
        v = stash[s, k] + pt[s % 2, k].astype(F32)

        @pl.when(is_end & (s >= 1))
        def _():
            rs[s, k] = v.astype(BF16)

        @pl.when(is_mid | (s == 0))
        def _():
            stash[s, k] = v

    def end_send(s, k):
        @pl.when(is_end & (s >= 1))
        def _():
            send_rs(s, s, k, inward).start()

    def add_in(slot, s, k):
        rs_arrived(slot, k)
        rs[slot, k] = (stash[s, k] + rs[slot, k].astype(F32)).astype(BF16)

    def second(k):
        @pl.when(k >= 1)
        def _():
            send_rs(2, 4, k - 1, inward).start()

        add_in(2, 1, k)

    x_own = pltpu.make_async_copy(x_ref, xb.at[pl.ds(0, R)], xsem.at[0])
    x_own.start()
    pl.semaphore_wait(barrier, 2 + mid)

    @pl.loop(0, NP)
    def _(p):
        own_x(p, 0).start()
        own_x(p, 1).start()

        @pl.when(is_mid)
        def _():
            own_x(p, 2).start()

    wait_partner_x(z)
    x_load_partner(z).start()
    x_own.wait()
    x_load_partner(z).wait()

    @pl.loop(0, 4)
    def _(s):
        base = s * TOT

        @pl.loop(0, NG)
        def _(i):
            g = base + 2 * i
            s0, s1 = lax.rem(g, NS), lax.rem(g + 1, NS)
            fetch(g + NS - 1)
            gu_copy(wg_ref, i, 0, s0, 0).wait()
            gu_copy(wu_ref, i, 0, s0, 1).wait()
            acc[...] = jnp.dot(xb[:, :KH], ring[s0], preferred_element_type=F32)
            fetch(g + NS)
            gu_copy(wg_ref, i, 1, s1, 0).wait()
            gu_copy(wu_ref, i, 1, s1, 1).wait()
            t = acc[...] + jnp.dot(xb[:, KH:], ring[s1], preferred_element_type=F32)
            hid[:, pl.ds(pl.multiple_of(i * GW, GW), GW)] = (
                jax.nn.silu(t[:, :GW]) * t[:, GW:]).astype(BF16)

            @pl.when((i == 3) | (i == 6))
            def _():
                relay(s, i // 3 - 1)

            @pl.when(is_mid & (s == 2) & (i == 3))
            def _():
                relay(jnp.int32(1), jnp.int32(4))

            @pl.when(is_mid & (s == 3) & (i >= 2))
            def _():
                second(i - 2)

        early = is_mid & ((s == 1) | (s == 2))
        nxt = real(block(s + 1))

        @pl.when(early)
        def _():
            wait_partner_x(nxt)
            x_load_own(nxt).start()
            x_load_partner(nxt).start()

        @pl.loop(0, ND)
        def _(j):
            g = base + 2 * NG + j
            s0 = lax.rem(g, NS)
            fetch(g + NS - 1)
            d_copy(j, s0).wait()
            t = jnp.dot(hid[...], ring[s0, :F], preferred_element_type=F32)

            @pl.when(j >= PS)
            def _():
                send_pt(s, j - PS).wait_send()

            stash[s, j] = t[:R]
            pst[j % PS] = t[R:].astype(BF16)

            @pl.when(j >= 1)
            def _():
                send_pt(s, j - 1).start()

            @pl.when(j >= LAG + 1)
            def _():
                end_send(s, j - LAG - 1)

            @pl.when(j >= LAG)
            def _():
                fold(s, j - LAG)

            @pl.when((j == 2) | (j == 11))
            def _():
                relay(s, 2 + j // 11)

            @pl.when(is_mid & (s == 3) & (j >= 2) & (j % 2 == 0))
            def _():
                second(NG - 2 + j // 2 - 1)

        send_pt(s, ND - 1).start()
        end_send(s, ND - LAG - 1)

        @pl.when(is_end | (s == 0))
        def _():
            relay(s, jnp.int32(4))

        @pl.when((s < 3) & jnp.logical_not(early))
        def _():
            x_load_own(nxt).start()

        @pl.loop(ND - LAG, ND)
        def _(k):
            fold(s, k)

        @pl.when((s < 3) & jnp.logical_not(early))
        def _():
            wait_partner_x(nxt)
            x_load_partner(nxt).start()

        @pl.loop(ND - LAG, ND)
        def _(k):
            end_send(s, k)

        @pl.loop(ND - PS, ND)
        def _(k):
            send_pt(s, k).wait_send()

        @pl.when(s < 3)
        def _():
            x_load_own(nxt).wait()
            x_load_partner(nxt).wait()

    def y_copy(slot, k):
        return pltpu.make_async_copy(
            rs.at[slot, k], y_ref.at[:, pl.ds(pl.multiple_of(k * DW, DW), DW)], ysem.at[k])

    @pl.when(is_mid)
    def _():
        send_rs(2, 4, ND - 1, inward).start()

        @pl.loop(0, ND + 1)
        def _(k):
            @pl.when(k < ND)
            def _():
                add_in(3, 3, k)
                rs_arrived(1, k)
                rs_arrived(4, k)
                rs[1, k] = (stash[0, k] + rs[1, k].astype(F32) + rs[4, k].astype(F32)).astype(BF16)
                send_rs(3, 0, k, inward).start()

            @pl.when(k >= 1)
            def _():
                y_copy(1, k - 1).start()
                add_in(0, 2, k - 1)

            @pl.when(k >= 2)
            def _():
                send_rs(0, 0, k - 2, outward).start()

        send_rs(0, 0, ND - 1, outward).start()

        @pl.loop(0, ND)
        def _(k):
            y_copy(1, k).wait()
            send_rs(2, 4, k, inward).wait_send()
            send_rs(3, 0, k, inward).wait_send()
            send_rs(0, 0, k, outward).wait_send()

    @pl.when(is_end)
    def _():
        @pl.loop(0, ND)
        def _(k):
            add_in(0, 0, k)

            @pl.when(k >= 1)
            def _():
                y_copy(0, k - 1).start()

        y_copy(0, ND - 1).start()

        @pl.loop(0, ND)
        def _(k):
            y_copy(0, k).wait()
            for s in (1, 2, 3):
                send_rs(s, s, k, inward).wait_send()

    @pl.loop(0, NP)
    def _(p):
        own_x(p, 0).wait_send()
        own_x(p, 1).wait_send()

        @pl.when(is_mid)
        def _():
            own_x(p, 2).wait_send()
            for bb in (0, 2, 3):
                forward(real(bb), p, inward).wait_send()
                share(real(bb), p).wait_send()

        @pl.when(is_end)
        def _():
            for bb in (1, 2, 3):
                share(real(bb), p).wait_send()


def solution(mesh):
    dma = pltpu.SemaphoreType.DMA

    def step(x, w_gate, w_up, w_down):
        hbm = pl.BlockSpec(memory_space=pltpu.HBM)
        y, _ = pl.pallas_call(
            kernel,
            name="mlp",
            out_shape=(jax.ShapeDtypeStruct((R, D), BF16),
                       jax.ShapeDtypeStruct((4, 2, R, D), BF16)),
            in_specs=[hbm] * 4,
            out_specs=(hbm, hbm),
            scratch_shapes=[
                pltpu.VMEM((2 * R, D), BF16),
                pltpu.VMEM((NS, KH, DW), BF16),
                pltpu.VMEM((2 * R, F), BF16),
                pltpu.VMEM((2 * R, 2 * GW), F32),
                pltpu.VMEM((4, ND, R, DW), F32),
                pltpu.VMEM((PS, R, DW), BF16),
                pltpu.VMEM((2, ND, R, DW), BF16),
                pltpu.VMEM((5, ND, R, DW), BF16),
                dma((NS, 2)), dma((2,)),
                dma((4, NP)), dma((4, NP)), dma((4, NP)), dma((4, NP)), dma((4, NP)),
                dma((PS,)), dma((2, ND)), dma((4, ND)), dma((5, ND)), dma((ND,)),
            ],
            compiler_params=pltpu.CompilerParams(
                collective_id=0, has_side_effects=True, vmem_limit_bytes=67043328),
        )(x, w_gate, w_up, w_down)
        return y

    return jax.shard_map(
        step,
        mesh=mesh,
        in_specs=(P(("dp", "tp"), None), P(None, "tp"), P(None, "tp"), P("tp", None)),
        out_specs=P(("dp", "tp"), None),
        check_vma=False,
    )
```

```python
import jax
import jax.numpy as jnp
from jax import lax
from jax.experimental import pallas as pl
from jax.experimental.pallas import tpu as pltpu
from jax.sharding import PartitionSpec as P

MESH = pl.DeviceIdType.MESH
F32, BF16 = jnp.float32, jnp.bfloat16

D = 7168
F = 2560
R = 160
NP = 4
KC = D // NP
GW, NG = 512, F // 512
DW, ND = 512, D // 512
ND2, FH = ND // 2, F // 2
GU = NP * NG
TOT = GU + ND
NS = 5
PS = 4


def kernel(x_ref, wg_ref, wu_ref, wd_ref, y_ref, xg, xb, ring, hid, acc, stash, pst, pt, rs,
           wsem, xsem, ag_recv, agp_recv, fwd_send, out_send, d2d_send,
           pst_send, pt_recv, rs_send, rs_recv, ysem):
    tp = lax.axis_index("tp")
    z, c = tp // 2, tp % 2
    mir = z // 2
    mid = (z * (3 - z)) // 2
    is_mid, is_end = mid == 1, mid == 0
    din = 1 - 2 * mir
    partner = {"tp": 2 * z + (1 - c)}
    inward = {"tp": 2 * (z + din) + c}
    outward = {"tp": 2 * (z - din * mid) + c}

    def real(bb):
        return bb + mir * (3 - 2 * bb)

    def block(s):
        m = ((s + 1) % 3) * (1 - s // 3) + 3 * (s // 3)
        return mid * m + (1 - mid) * s

    barrier = pltpu.get_barrier_semaphore()
    pl.semaphore_signal(barrier, inc=1, device_id=partner, device_id_type=MESH)
    pl.semaphore_signal(barrier, inc=1, device_id=inward, device_id_type=MESH)

    @pl.when(is_mid)
    def _():
        pl.semaphore_signal(barrier, inc=1, device_id=outward, device_id_type=MESH)

    def gu_copy(ref, u, slot, h):
        return pltpu.make_async_copy(
            ref.at[pl.ds(pl.multiple_of((u // NG) * KC, KC), KC),
                   pl.ds(pl.multiple_of((u % NG) * GW, GW), GW)],
            ring.at[slot, :, pl.ds(h * GW, GW)], wsem.at[slot, h])

    def d_copy(j, slot):
        return pltpu.make_async_copy(
            wd_ref.at[pl.ds(pl.multiple_of((j % 2) * FH, FH), FH),
                      pl.ds(pl.multiple_of((j // 2) * 2 * DW, 2 * DW), 2 * DW)],
            ring.at[slot, pl.ds(0, FH)], wsem.at[slot, 0])

    def fetch(g):
        slot = lax.rem(g, NS)
        r = lax.rem(g + ND, TOT)
        last = GU + 3 * TOT

        def gate_up(u):
            gu_copy(wg_ref, u, slot, 0).start()
            gu_copy(wu_ref, u, slot, 1).start()

        @pl.when(g < GU)
        def _():
            gate_up(g)

        @pl.when((g >= GU) & (g < last) & (r < GU))
        def _():
            gate_up(r)

        @pl.when((g >= GU) & (g < last) & (r >= GU))
        def _():
            d_copy(r - GU, slot).start()

        @pl.when((g >= last) & (g < last + ND))
        def _():
            d_copy(r, slot).start()

    for k in range(NS - 1):
        fetch(jnp.int32(k))

    def send_x(src, b, p, sem, recv, dev):
        return pltpu.make_async_remote_copy(
            src_ref=src, dst_ref=xg.at[b, c, p], send_sem=sem.at[b, p],
            recv_sem=recv.at[b, p], device_id=dev, device_id_type=MESH)

    def own_cols(p):
        return x_ref.at[:, pl.ds(pl.multiple_of(p * KC, KC), KC)]

    def own_x(p, kind):
        if kind == 0:
            return send_x(own_cols(p), z, p, d2d_send, agp_recv, partner)
        if kind == 1:
            return send_x(own_cols(p), z, p, fwd_send, ag_recv, inward)
        return send_x(own_cols(p), z, p, out_send, ag_recv, outward)

    def arrived(b, p):
        with jax.named_scope("w_ag"):
            send_x(xg.at[b, c, p], b, p, fwd_send, ag_recv, partner).wait_recv()

    def forward(b, p, dev):
        return send_x(xg.at[b, c, p], b, p, fwd_send, ag_recv, dev)

    def share(b, p):
        return send_x(xg.at[b, c, p], b, p, d2d_send, agp_recv, partner)

    def load_own(b, p):
        return pltpu.make_async_copy(xg.at[b, c, p], xb.at[p, pl.ds(0, R)], xsem.at[0, p])

    def load_partner(b, p):
        return pltpu.make_async_copy(xg.at[b, 1 - c, p], xb.at[p, pl.ds(R, R)], xsem.at[1, p])

    def partner_piece(b, p):
        with jax.named_scope("w_px"):
            pltpu.make_async_remote_copy(
                src_ref=xg.at[b, 1 - c, p], dst_ref=xg.at[b, 1 - c, p],
                send_sem=d2d_send.at[b, p], recv_sem=agp_recv.at[b, p],
                device_id=partner, device_id_type=MESH).wait_recv()
        load_partner(b, p).start()

    def relay_first(p):
        b = real(1 + mid)
        arrived(b, p)

        @pl.when(is_mid)
        def _():
            forward(b, p, outward).start()

        share(b, p).start()
        load_own(b, p).start()

        @pl.when(is_mid)
        def _():
            b0 = real(0)
            arrived(b0, p)
            forward(b0, p, inward).start()
            share(b0, p).start()

    def partner_first(p):
        partner_piece(real(1 + mid), p)

    def relay_end(bb, p):
        @pl.when(is_end)
        def _():
            arrived(real(bb), p)
            share(real(bb), p).start()
            load_own(real(bb), p).start()

    def partner_end(bb, p):
        @pl.when(is_end)
        def _():
            partner_piece(real(bb), p)

    def relay_mid(p):
        @pl.when(is_mid)
        def _():
            arrived(real(3), p)
            forward(real(3), p, outward).start()
            share(real(3), p).start()

    def load_mid(bb):
        @pl.when(is_mid)
        def _():
            @pl.loop(0, NP)
            def _(p):
                load_own(real(bb), p).start()
                partner_piece(real(bb), p)

    def send_pt(s, j):
        k = (ND * (s - 1) + j) % PS
        return pltpu.make_async_remote_copy(
            src_ref=pst.at[k], dst_ref=pt.at[k], send_sem=pst_send.at[k],
            recv_sem=pt_recv.at[k], device_id=partner, device_id_type=MESH)

    def send_rs(slot, there, j, dev):
        return pltpu.make_async_remote_copy(
            src_ref=rs.at[slot, j], dst_ref=rs.at[there, j], send_sem=rs_send.at[slot, j],
            recv_sem=rs_recv.at[there, j], device_id=dev, device_id_type=MESH)

    def rs_arrived(slot, j):
        with jax.named_scope("w_rs"):
            send_rs(0, slot, j, inward).wait_recv()

    def fold(s, k):
        with jax.named_scope("w_pt"):
            send_pt(s, k).wait_recv()
        v = stash[s % 4, k] + pt[(ND * (s - 1) + k) % PS].astype(F32)

        @pl.when(is_end & (s < 4))
        def _():
            rs[s, k] = v.astype(BF16)

        @pl.when(is_mid | (s == 4))
        def _():
            stash[s % 4, k] = v

    def end_send(s, k):
        @pl.when(is_end & (s < 4))
        def _():
            send_rs(s, s, k, inward).start()

    def add_in(slot, s, k):
        rs_arrived(slot, k)
        rs[slot, k] = (stash[s, k] + rs[slot, k].astype(F32)).astype(BF16)

    def pass_on(k):
        @pl.when(k < ND)
        def _():
            send_rs(2, 4, k, inward).start()

        @pl.when(k >= ND)
        def _():
            send_rs(3, 0, k - ND, inward).start()

    def take(k):
        @pl.when(k < ND)
        def _():
            add_in(2, 1, k)

        @pl.when(k >= ND)
        def _():
            add_in(3, 3, k - ND)

    def x_own(p):
        return pltpu.make_async_copy(own_cols(p), xb.at[p, pl.ds(0, R)], xsem.at[0, p])

    for p in range(NP):
        x_own(p).start()
    with jax.named_scope("w_bar"):
        pl.semaphore_wait(barrier, 2 + mid)

    @pl.loop(0, NP)
    def _(p):
        own_x(p, 0).start()
        own_x(p, 1).start()

        @pl.when(is_mid)
        def _():
            own_x(p, 2).start()

    @pl.loop(0, NP)
    def _(p):
        partner_piece(z, p)

    @pl.loop(0, 5)
    def _(s):
        base = (GU + (s - 1) * TOT) * ((s + 3) // 4)

        @pl.when(s < 4)
        def _():
            @pl.loop(0, GU)
            def _(q):
                kc, n = q // NG, q % NG

                @pl.when(n == 0)
                def _():
                    with jax.named_scope("w_xl"):
                        load_own(z, kc).wait()
                        load_partner(z, kc).wait()

                g = base + q
                slot = lax.rem(g, NS)

                @pl.when((q == 0) & (s >= 2))
                def _():
                    fetch(g + NS - 2)

                fetch(g + NS - 1)
                with jax.named_scope("w_wg"):
                    gu_copy(wg_ref, q, slot, 0).wait()
                    gu_copy(wu_ref, q, slot, 1).wait()

                @pl.when(kc == 0)
                def _():
                    with jax.named_scope("gu"):
                        acc[n] = jnp.dot(xb[kc], ring[slot], preferred_element_type=F32)

                @pl.when((kc > 0) & (kc < NP - 1))
                def _():
                    with jax.named_scope("gu"):
                        acc[n] += jnp.dot(xb[kc], ring[slot], preferred_element_type=F32)

                @pl.when(kc == NP - 1)
                def _():
                    with jax.named_scope("gu"):
                        t = acc[n] + jnp.dot(xb[kc], ring[slot], preferred_element_type=F32)
                        hid[(s + 3) // 4, :, pl.ds(pl.multiple_of(n * GW, GW), GW)] = (
                            jax.nn.silu(t[:, :GW]) * t[:, GW:]).astype(BF16)

                @pl.when(s == 0)
                def _():
                    @pl.when((q == 9) | (q == 18))
                    def _():
                        relay_first(q // 18)

                    @pl.when((q == 11) | (q == 19))
                    def _():
                        partner_first(q // 18)

                @pl.when((s == 1) & ((q == 3) | (q == 10)))
                def _():
                    relay_first(2 + q // 10)

                @pl.when((s == 1) & ((q == 5) | (q == 12)))
                def _():
                    partner_first(2 + q // 10)

                @pl.when(s >= 2)
                def _():
                    @pl.when((q == 3) | (q == 11))
                    def _():
                        relay_end(s, 2 + q // 10)

                    @pl.when((q == 5) | (q == 13))
                    def _():
                        partner_end(s, 2 + q // 10)

                    @pl.when((s == 2) & ((q == 3) | (q == 14)))
                    def _():
                        relay_mid(2 + q // 10)

                    @pl.when(is_mid & (s == 3))
                    def _():
                        m = q % 7

                        @pl.when((m == 1) | (m == 3) | (m == 6))
                        def _():
                            pass_on(2 + 3 * (q // 7) + m // 3)

                        @pl.when((m == 0) | (m == 2) | (m == 5))
                        def _():
                            take(2 + 3 * (q // 7) + (m + 1) // 3)

        @pl.when(s > 0)
        def _():
            @pl.when((s == 1) | (s == 2))
            def _():
                load_mid(2 * s - 2 + s // 2)

            @pl.when(is_mid & (s == 3))
            def _():
                pass_on(jnp.int32(10))

            @pl.loop(0, ND2)
            def _(j):
                g = base + GU * (1 - s // 4) + 2 * j
                s0, s1 = lax.rem(g, NS), lax.rem(g + 1, NS)

                @pl.when((j > 0) | (s == 4))
                def _():
                    fetch(g + NS - 2)

                fetch(g + NS - 1)
                with jax.named_scope("w_wd"):
                    d_copy(2 * j, s0).wait()
                    d_copy(2 * j + 1, s1).wait()

                @pl.when(j >= 2)
                def _():
                    for h in range(2):
                        send_pt(s, 2 * j - PS + h).wait_send()

                hs = 1 - s // 4
                for h in range(2):
                    with jax.named_scope("d"):
                        cols = slice(h * DW, (h + 1) * DW)
                        t = jnp.dot(hid[hs, :, :FH], ring[s0, :FH, cols],
                                    preferred_element_type=F32)
                        t += jnp.dot(hid[hs, :, FH:], ring[s1, :FH, cols],
                                     preferred_element_type=F32)
                        stash[s % 4, 2 * j + h] = t[:R]
                        pst[(ND * (s - 1) + 2 * j + h) % PS] = t[R:].astype(BF16)

                def for_middle(do):
                    @pl.when((s == 2) & (j >= 5))
                    def _():
                        do(j - 5)

                    @pl.when((s == 3) & (j != 3) & (j < 6))
                    def _():
                        do(11 + j - j // 4)

                    @pl.when((s == 4) & (j % 3 != 2))
                    def _():
                        do(16 + j - (j + 1) // 3)

                def for_outer(do):
                    @pl.when(is_mid & (s == 4) & (j % 3 != 0))
                    def _():
                        do(j - 1 - j // 3)

                @pl.when(is_mid)
                def _():
                    for_middle(take)

                for_outer(lambda k: add_in(0, 2, k))

                @pl.when(j >= 1)
                def _():
                    fold(s, 2 * j - 2)
                    fold(s, 2 * j - 1)

                for h in range(2):
                    send_pt(s, 2 * j + h).start()

                @pl.when(j >= 1)
                def _():
                    end_send(s, 2 * j - 2)
                    end_send(s, 2 * j - 1)

                @pl.when(is_mid)
                def _():
                    for_middle(pass_on)

                for_outer(lambda k: send_rs(0, 0, k, outward).start())

                @pl.when((s == 1) | (s == 2))
                def _():
                    @pl.when((j == 0) | (j == 4))
                    def _():
                        relay_end(s + 1, j // 4)

                    @pl.when((j == 1) | (j == 5))
                    def _():
                        partner_end(s + 1, j // 4)

                    @pl.when((s == 1) & ((j == 0) | (j == 4)))
                    def _():
                        relay_mid(j // 4)

            fold(s, ND - 2)
            fold(s, ND - 1)

            @pl.loop(ND - PS, ND)
            def _(k):
                send_pt(s, k).wait_send()

            end_send(s, ND - 2)
            end_send(s, ND - 1)

    def y_copy(slot, k):
        return pltpu.make_async_copy(
            rs.at[slot, k], y_ref.at[:, pl.ds(pl.multiple_of(k * DW, DW), DW)], ysem.at[k])

    @pl.when(is_mid)
    def _():
        def finish(k):
            rs_arrived(1, k)
            rs_arrived(4, k)
            rs[1, k] = (stash[0, k] + rs[1, k].astype(F32) + rs[4, k].astype(F32)).astype(BF16)

        @pl.loop(0, ND - 4)
        def _(i):
            add_in(0, 2, 4 + i)

            @pl.when(i < ND2)
            def _():
                finish(2 * i)

            send_rs(0, 0, 4 + i, outward).start()

            @pl.when(i < ND2)
            def _():
                add_in(3, 3, 7 + i)
                finish(2 * i + 1)
                send_rs(3, 0, 7 + i, inward).start()
                y_copy(1, 2 * i).start()

            @pl.when((i > 0) & (i <= ND2))
            def _():
                y_copy(1, 2 * i - 1).start()

        @pl.loop(0, ND)
        def _(k):
            y_copy(1, k).wait()
            send_rs(2, 4, k, inward).wait_send()
            send_rs(3, 0, k, inward).wait_send()
            send_rs(0, 0, k, outward).wait_send()

    @pl.when(is_end)
    def _():
        @pl.loop(0, ND)
        def _(k):
            add_in(0, 0, k)

            @pl.when(k >= 1)
            def _():
                y_copy(0, k - 1).start()

        y_copy(0, ND - 1).start()

        @pl.loop(0, ND)
        def _(k):
            y_copy(0, k).wait()
            for s in (1, 2, 3):
                send_rs(s, s, k, inward).wait_send()

    @pl.loop(0, NP)
    def _(p):
        own_x(p, 0).wait_send()
        own_x(p, 1).wait_send()

        @pl.when(is_mid)
        def _():
            own_x(p, 2).wait_send()
            for bb in (0, 2, 3):
                forward(real(bb), p, inward).wait_send()
                share(real(bb), p).wait_send()

        @pl.when(is_end)
        def _():
            for bb in (1, 2, 3):
                share(real(bb), p).wait_send()


def solution(mesh):
    dma = pltpu.SemaphoreType.DMA

    def step(x, w_gate, w_up, w_down):
        hbm = pl.BlockSpec(memory_space=pltpu.HBM)
        y, _ = pl.pallas_call(
            kernel,
            name="mlp",
            out_shape=(jax.ShapeDtypeStruct((R, D), BF16),
                       jax.ShapeDtypeStruct((4, 2, NP, R, KC), BF16)),
            in_specs=[hbm] * 4,
            out_specs=(hbm, hbm),
            scratch_shapes=[
                pltpu.VMEM((NP, 2 * R, KC), BF16),
                pltpu.VMEM((NS, KC, 2 * GW), BF16),
                pltpu.VMEM((2, 2 * R, F), BF16),
                pltpu.VMEM((NG, 2 * R, 2 * GW), F32),
                pltpu.VMEM((4, ND, R, DW), F32),
                pltpu.VMEM((PS, R, DW), BF16),
                pltpu.VMEM((PS, R, DW), BF16),
                pltpu.VMEM((5, ND, R, DW), BF16),
                dma((NS, 2)), dma((2, NP)),
                dma((4, NP)), dma((4, NP)), dma((4, NP)), dma((4, NP)), dma((4, NP)),
                dma((PS,)), dma((PS,)), dma((4, ND)), dma((5, ND)), dma((ND,)),
            ],
            compiler_params=pltpu.CompilerParams(
                collective_id=0, has_side_effects=True, vmem_limit_bytes=67043328),
        )(x, w_gate, w_up, w_down)
        return y

    return jax.shard_map(
        step,
        mesh=mesh,
        in_specs=(P(("dp", "tp"), None), P(None, "tp"), P(None, "tp"), P("tp", None)),
        out_specs=P(("dp", "tp"), None),
        check_vma=False,
    )
```

```python
import functools

import jax
import jax.numpy as jnp
from jax import lax
from jax.experimental import pallas as pl
from jax.experimental.pallas import tpu as pltpu
from jax.sharding import PartitionSpec as P

MESH = pl.DeviceIdType.MESH
F32, BF16 = jnp.float32, jnp.bfloat16

D = 7168
F = 2560
R = 160
NP = 4
KC = D // NP
GW, NG = 512, F // 512
DW, ND = 512, D // 512
ND2, FH = ND // 2, F // 2
GU = NP * NG
NS = 5
TAKES = (0, 2, 4, 6, 8, 11, 13, 15, 18)
PS = 4


def kernel(x_ref, wg_ref, wu_ref, wd_ref, y_ref, xg, xb, ring, hid, acc, stash, pst, pt, rs,
           wsem, xsem, ag_recv, agp_recv, fwd_send, out_send, d2d_send,
           pst_send, pt_recv, rs_send, rs_recv, ysem):
    tp = lax.axis_index("tp")
    z, c = tp // 2, tp % 2
    mir = z // 2
    mid = (z * (3 - z)) // 2
    is_mid, is_end = mid == 1, mid == 0
    din = 1 - 2 * mir
    partner = {"tp": 2 * z + (1 - c)}
    inward = {"tp": 2 * (z + din) + c}
    outward = {"tp": 2 * (z - din * mid) + c}

    def real(bb):
        return bb + mir * (3 - 2 * bb)

    barrier = pltpu.get_barrier_semaphore()
    pl.semaphore_signal(barrier, inc=1, device_id=partner, device_id_type=MESH)
    pl.semaphore_signal(barrier, inc=1, device_id=inward, device_id_type=MESH)

    @pl.when(is_mid)
    def _():
        pl.semaphore_signal(barrier, inc=1, device_id=outward, device_id_type=MESH)

    def gu_copy(ref, u, slot, h):
        return pltpu.make_async_copy(
            ref.at[pl.ds(pl.multiple_of((u // NG) * KC, KC), KC),
                   pl.ds(pl.multiple_of((u % NG) * GW, GW), GW)],
            ring.at[slot, :, pl.ds(h * GW, GW)], wsem.at[slot, h])

    def fetch_gu(u, slot):
        gu_copy(wg_ref, u, slot, 0).start()
        gu_copy(wu_ref, u, slot, 1).start()

    def d_copy(d, slot):
        return pltpu.make_async_copy(
            wd_ref.at[pl.ds(pl.multiple_of((d % 2) * FH, FH), FH),
                      pl.ds(pl.multiple_of((d // 2) * 2 * DW, 2 * DW), 2 * DW)],
            ring.at[slot, pl.ds(0, FH)], wsem.at[slot, 0])

    def fetch_d(d):
        d_copy(d, lax.rem(d, NS)).start()

    for u in range(NS - 1):
        fetch_gu(u, u)

    def send_x(src, b, p, sem, recv, dev):
        return pltpu.make_async_remote_copy(
            src_ref=src, dst_ref=xg.at[b, c, p], send_sem=sem.at[b, p],
            recv_sem=recv.at[b, p], device_id=dev, device_id_type=MESH)

    def own_cols(p):
        return x_ref.at[:, pl.ds(pl.multiple_of(p * KC, KC), KC)]

    def own_x(p, kind):
        if kind == 0:
            return send_x(own_cols(p), z, p, d2d_send, agp_recv, partner)
        if kind == 1:
            return send_x(own_cols(p), z, p, fwd_send, ag_recv, inward)
        return send_x(own_cols(p), z, p, out_send, ag_recv, outward)

    def arrived(b, p):
        with jax.named_scope("w_ag"):
            send_x(xg.at[b, c, p], b, p, fwd_send, ag_recv, partner).wait_recv()

    def forward(b, p, dev):
        return send_x(xg.at[b, c, p], b, p, fwd_send, ag_recv, dev)

    def share(b, p):
        return send_x(xg.at[b, c, p], b, p, d2d_send, agp_recv, partner)

    def load_own(b, p):
        return pltpu.make_async_copy(xg.at[b, c, p], xb.at[p, pl.ds(0, R)], xsem.at[0, p])

    def load_partner(b, p):
        return pltpu.make_async_copy(xg.at[b, 1 - c, p], xb.at[p, pl.ds(R, R)], xsem.at[1, p])

    def partner_piece(b, p):
        with jax.named_scope("w_px"):
            pltpu.make_async_remote_copy(
                src_ref=xg.at[b, 1 - c, p], dst_ref=xg.at[b, 1 - c, p],
                send_sem=d2d_send.at[b, p], recv_sem=agp_recv.at[b, p],
                device_id=partner, device_id_type=MESH).wait_recv()
        load_partner(b, p).start()

    def relay_first(p):
        b = real(1 - mid)
        arrived(b, p)

        @pl.when(is_mid)
        def _():
            forward(b, p, inward).start()

        share(b, p).start()
        load_own(b, p).start()

    def partner_first(p):
        partner_piece(real(1 - mid), p)

    def relay_end(s, p):
        arrived(real(5 - s), p)
        share(real(5 - s), p).start()
        load_own(real(5 - s), p).start()

    def partner_end(s, p):
        partner_piece(real(5 - s), p)

    def relay_mid(bb, p):
        arrived(real(bb), p)
        forward(real(bb), p, outward).start()
        share(real(bb), p).start()

    def load_mid(bb):
        @pl.loop(0, NP)
        def _(p):
            load_own(real(bb), p).start()
            partner_piece(real(bb), p)

    def send_pt(s, j):
        k = (ND * (s - 1) + j) % PS
        return pltpu.make_async_remote_copy(
            src_ref=pst.at[k], dst_ref=pt.at[k], send_sem=pst_send.at[k],
            recv_sem=pt_recv.at[k], device_id=partner, device_id_type=MESH)

    def send_rs(slot, there, j, dev):
        return pltpu.make_async_remote_copy(
            src_ref=rs.at[slot, j], dst_ref=rs.at[there, j], send_sem=rs_send.at[slot, j],
            recv_sem=rs_recv.at[there, j], device_id=dev, device_id_type=MESH)

    def rs_arrived(slot, j):
        with jax.named_scope(f"w_rs{slot}"):
            send_rs(0, slot, j, inward).wait_recv()

    def fold(s, k):
        with jax.named_scope("w_pt"):
            send_pt(s, k).wait_recv()
        v = stash[s % 4, k] + pt[(ND * (s - 1) + k) % PS].astype(F32)

        @pl.when(is_end & (s < 4))
        def _():
            rs[s, k] = v.astype(BF16)

        @pl.when(is_mid | (s == 4))
        def _():
            stash[s % 4, k] = v

    def end_send(s, k):
        @pl.when(is_end & (s < 4))
        def _():
            send_rs(s, s, k, inward).start()

    def add_in(slot, s, k):
        rs_arrived(slot, k)
        rs[slot, k] = (stash[s, k] + rs[slot, k].astype(F32)).astype(BF16)

    def pass_on(k):
        @pl.when(k < ND)
        def _():
            send_rs(2, 0, k, inward).start()

        @pl.when(k >= ND)
        def _():
            send_rs(3, 4, k - ND, inward).start()

    def take(k):
        @pl.when(k < ND)
        def _():
            add_in(2, 2, k)

        @pl.when(k >= ND)
        def _():
            add_in(3, 3, k - ND)

    def x_own(p):
        return pltpu.make_async_copy(own_cols(p), xb.at[p, pl.ds(0, R)], xsem.at[0, p])

    for p in range(NP):
        x_own(p).start()
    with jax.named_scope("w_bar"):
        pl.semaphore_wait(barrier, 2 + mid)

    @pl.loop(0, NP)
    def _(p):
        own_x(p, 0).start()

        @pl.when(is_end | (p == 0))
        def _():
            own_x(p, 1).start()

        @pl.when(is_mid)
        def _():
            own_x(p, 2).start()

    partner_piece(z, 0)

    def gu_events(s, kc, n):
        def at(when, q, fn):
            if q // NG == kc:
                @pl.when(when & (n == q % NG))
                def _():
                    fn()

        first, second, both = s == 0, s == 1, (s == 2) | (s == 3)
        for p in range(1, NP):
            at(first, p - 1, functools.partial(partner_piece, z, p))
        at(first, 9, lambda: relay_first(0))
        at(first, 11, lambda: partner_first(0))
        at(first, 18, lambda: relay_first(1))
        at(first, 19, lambda: partner_first(1))
        at(first & is_mid, 19, lambda: relay_mid(3, 0))
        at(second, 5, lambda: relay_first(2))
        at(second, 7, lambda: partner_first(2))
        at(second & is_mid, 10, lambda: relay_mid(3, 1))
        at(second, 12, lambda: relay_first(3))

        def own_rest():
            for p in range(1, NP):
                own_x(p, 1).start()

        at(second & is_mid, 12, own_rest)
        at(second, 14, lambda: partner_first(3))
        at(second & is_mid, 18, lambda: relay_mid(3, 2))
        for i, q in enumerate((0, 7, 15)):
            at((s == 2) & is_mid, q, functools.partial(relay_mid, 2, 1 + i))
        at(both & is_end, 1, lambda: partner_end(s, 1))
        at(both & is_end, 6, lambda: relay_end(s, 2))
        at(both & is_end, 8, lambda: partner_end(s, 2))
        at(both & is_end, 12, lambda: relay_end(s, 3))
        at(both & is_end, 14, lambda: partner_end(s, 3))
        for i, q in enumerate(TAKES):
            at((s == 3) & is_mid, q, functools.partial(take, jnp.int32(3 + i)))

    def gu_sends(s, kc, n):
        for i, q in enumerate(TAKES):
            if (q + 1) // NG == kc:
                @pl.when((s == 3) & is_mid & (n == (q + 1) % NG))
                def _():
                    pass_on(jnp.int32(3 + i))

    @pl.loop(0, 5)
    def _(s):
        @pl.when(s < 4)
        def _():
            @pl.when(s >= 2)
            def _():
                fetch_gu(2, 2)
                fetch_gu(3, 3)

            for kc in range(NP):
                with jax.named_scope("w_xl"):
                    load_own(z, kc).wait()
                    load_partner(z, kc).wait()

                @pl.loop(0, NG)
                def _(n):
                    if kc < NP - 1:
                        fetch_gu(kc * NG + n + NS - 1, (n + NS - 1) % NS)
                    else:
                        @pl.when(n == 0)
                        def _():
                            fetch_gu(GU - 1, NS - 1)

                        @pl.when((n > 0) & (s == 0))
                        def _():
                            fetch_gu(n - 1, n - 1)

                        @pl.when((n > 0) & (s > 0))
                        def _():
                            fetch_d(n - 1)

                    gu_sends(s, kc, n)
                    with jax.named_scope("w_wg"):
                        gu_copy(wg_ref, kc * NG + n, n, 0).wait()
                        gu_copy(wu_ref, kc * NG + n, n, 1).wait()
                    with jax.named_scope("gu"):
                        t = jnp.dot(xb[kc], ring[n], preferred_element_type=F32)
                        if kc == 0:
                            acc[n] = t
                        elif kc < NP - 1:
                            acc[n] += t
                        else:
                            t += acc[n]
                            hid[(s + 3) // 4, :, pl.ds(pl.multiple_of(n * GW, GW), GW)] = (
                                jax.nn.silu(t[:, :GW]) * t[:, GW:]).astype(BF16)
                    gu_events(s, kc, n)

        @pl.when(s > 0)
        def _():
            @pl.when(is_mid & (s >= 3))
            def _():
                take(12 + 5 * (s - 3))

            @pl.loop(0, ND2)
            def _(j):
                s0, s1 = lax.rem(2 * j, NS), lax.rem(2 * j + 1, NS)

                @pl.when(j == 0)
                def _():
                    @pl.when(s == 4)
                    def _():
                        fetch_d(jnp.int32(2))
                        fetch_d(jnp.int32(3))

                    fetch_d(jnp.int32(4))

                @pl.when((j > 0) & (j < 6))
                def _():
                    fetch_d(2 * j + 3)

                @pl.when((j > 0) & (j < 5))
                def _():
                    fetch_d(2 * j + 4)

                @pl.when((j == 6) & (s < 3))
                def _():
                    fetch_gu(0, 0)
                    fetch_gu(1, 1)

                @pl.when((j == 6) & (s == 3))
                def _():
                    fetch_d(jnp.int32(0))
                    fetch_d(jnp.int32(1))

                @pl.when(is_mid & (s >= 3) & (j == 0))
                def _():
                    pass_on(12 + 5 * (s - 3))

                with jax.named_scope("w_wd"):
                    d_copy(2 * j, s0).wait()
                    d_copy(2 * j + 1, s1).wait()

                @pl.when(j >= 2)
                def _():
                    for h in range(2):
                        send_pt(s, 2 * j - PS + h).wait_send()

                hs = 1 - s // 4
                for h in range(2):
                    with jax.named_scope("d"):
                        cols = slice(h * DW, (h + 1) * DW)
                        t = jnp.dot(hid[hs, :, :FH], ring[s0, :FH, cols],
                                    preferred_element_type=F32)
                        t += jnp.dot(hid[hs, :, FH:], ring[s1, :FH, cols],
                                     preferred_element_type=F32)
                        stash[s % 4, 2 * j + h] = t[:R]
                        pst[(ND * (s - 1) + 2 * j + h) % PS] = t[R:].astype(BF16)

                def for_middle(do):
                    @pl.when((s == 2) & (j >= 3) & (j < 6))
                    def _():
                        do(j - 3)

                    @pl.when((s == 3) & (j % 3 != 2) & (j > 0))
                    def _():
                        do(12 + j - j // 3)

                    @pl.when((s == 4) & (j % 3 != 0))
                    def _():
                        do(17 + j - j // 3)

                def for_outer(do):
                    @pl.when(is_mid & (s >= 3))
                    def _():
                        do((s - 3) * ND2 + j)

                @pl.when(is_mid)
                def _():
                    for_middle(take)

                for_outer(lambda k: add_in(0, 1, k))

                @pl.when(j >= 1)
                def _():
                    fold(s, 2 * j - 2)
                    fold(s, 2 * j - 1)

                for h in range(2):
                    send_pt(s, 2 * j + h).start()

                @pl.when(j >= 1)
                def _():
                    end_send(s, 2 * j - 2)
                    end_send(s, 2 * j - 1)

                @pl.when(is_mid)
                def _():
                    for_middle(pass_on)

                for_outer(lambda k: send_rs(0, 0, k, outward).start())

                @pl.when((s == 1) | (s == 2))
                def _():
                    @pl.when(is_end & ((j == 0) | (j == 6)))
                    def _():
                        relay_end(s + 1, j // 6)

                    @pl.when(is_end & (j == 1))
                    def _():
                        partner_end(s + 1, 0)

                    @pl.when(is_mid & (s == 1) & (j == 3))
                    def _():
                        relay_mid(3, 3)
                        relay_mid(2, 0)

                    @pl.when(is_mid & (j == 5))
                    def _():
                        load_mid(4 - s)

            fold(s, ND - 2)
            fold(s, ND - 1)

            @pl.loop(ND - PS, ND)
            def _(k):
                send_pt(s, k).wait_send()

            end_send(s, ND - 2)
            end_send(s, ND - 1)

    def y_copy(slot, k):
        return pltpu.make_async_copy(
            rs.at[slot, k], y_ref.at[:, pl.ds(pl.multiple_of(k * DW, DW), DW)], ysem.at[k])

    @pl.when(is_mid)
    def _():
        def finish(k):
            rs_arrived(1, k)
            rs_arrived(4, k)
            rs[1, k] = (stash[0, k] + rs[1, k].astype(F32) + rs[4, k].astype(F32)).astype(BF16)

        @pl.loop(0, ND2)
        def _(i):
            @pl.when(i < ND2 - 1)
            def _():
                add_in(3, 3, 8 + i)

            finish(2 * i)

            @pl.when(i < ND2 - 1)
            def _():
                send_rs(3, 4, 8 + i, inward).start()

            @pl.when(i > 0)
            def _():
                y_copy(1, 2 * i - 1).start()

            finish(2 * i + 1)
            y_copy(1, 2 * i).start()

        y_copy(1, ND - 1).start()

        @pl.loop(0, ND)
        def _(k):
            y_copy(1, k).wait()
            send_rs(2, 0, k, inward).wait_send()
            send_rs(3, 4, k, inward).wait_send()
            send_rs(0, 0, k, outward).wait_send()

    @pl.when(is_end)
    def _():
        @pl.loop(0, ND)
        def _(k):
            add_in(0, 0, k)

            @pl.when(k >= 1)
            def _():
                y_copy(0, k - 1).start()

        y_copy(0, ND - 1).start()

        @pl.loop(0, ND)
        def _(k):
            y_copy(0, k).wait()
            for s in (1, 2, 3):
                send_rs(s, s, k, inward).wait_send()

    @pl.loop(0, NP)
    def _(p):
        own_x(p, 0).wait_send()
        own_x(p, 1).wait_send()

        @pl.when(is_mid)
        def _():
            own_x(p, 2).wait_send()
            for bb in (0, 2, 3):
                forward(real(bb), p, inward).wait_send()
                share(real(bb), p).wait_send()

        @pl.when(is_end)
        def _():
            for bb in (1, 2, 3):
                share(real(bb), p).wait_send()


def solution(mesh):
    dma = pltpu.SemaphoreType.DMA

    def step(x, w_gate, w_up, w_down):
        hbm = pl.BlockSpec(memory_space=pltpu.HBM)
        y, _ = pl.pallas_call(
            kernel,
            name="mlp",
            out_shape=(jax.ShapeDtypeStruct((R, D), BF16),
                       jax.ShapeDtypeStruct((4, 2, NP, R, KC), BF16)),
            in_specs=[hbm] * 4,
            out_specs=(hbm, hbm),
            scratch_shapes=[
                pltpu.VMEM((NP, 2 * R, KC), BF16),
                pltpu.VMEM((NS, KC, 2 * GW), BF16),
                pltpu.VMEM((2, 2 * R, F), BF16),
                pltpu.VMEM((NG, 2 * R, 2 * GW), F32),
                pltpu.VMEM((4, ND, R, DW), F32),
                pltpu.VMEM((PS, R, DW), BF16),
                pltpu.VMEM((PS, R, DW), BF16),
                pltpu.VMEM((5, ND, R, DW), BF16),
                dma((NS, 2)), dma((2, NP)),
                dma((4, NP)), dma((4, NP)), dma((4, NP)), dma((4, NP)), dma((4, NP)),
                dma((PS,)), dma((PS,)), dma((4, ND)), dma((5, ND)), dma((ND,)),
            ],
            compiler_params=pltpu.CompilerParams(
                collective_id=0, has_side_effects=True, vmem_limit_bytes=67043328),
        )(x, w_gate, w_up, w_down)
        return y

    return jax.shard_map(
        step,
        mesh=mesh,
        in_specs=(P(("dp", "tp"), None), P(None, "tp"), P(None, "tp"), P("tp", None)),
        out_specs=P(("dp", "tp"), None),
        check_vma=False,
    )
```

```python
import functools

import jax
import jax.numpy as jnp
from jax import lax
from jax.experimental import pallas as pl
from jax.experimental.pallas import tpu as pltpu
from jax.sharding import PartitionSpec as P

MESH = pl.DeviceIdType.MESH
F32, BF16 = jnp.float32, jnp.bfloat16

D = 7168
F = 2560
R = 160
NP = 4
KC = D // NP
GW, NG = 512, F // 512
DW, ND = 512, D // 512
ND2, FH = ND // 2, F // 2
GU = NP * NG
NS = 5
TAKES = (0, 2, 4, 6, 8, 11, 13, 15, 18)
PS = 4


def kernel(x_ref, wg_ref, wu_ref, wd_ref, y_ref, xg, xb, ring, hid, acc, stash, pst, pt, rs,
           wsem, xsem, ag_recv, agp_recv, fwd_send, out_send, d2d_send,
           pst_send, pt_recv, rs_send, rs_recv):
    tp = lax.axis_index("tp")
    z, c = tp // 2, tp % 2
    mir = z // 2
    mid = (z * (3 - z)) // 2
    is_mid, is_end = mid == 1, mid == 0
    din = 1 - 2 * mir
    partner = {"tp": 2 * z + (1 - c)}
    inward = {"tp": 2 * (z + din) + c}
    outward = {"tp": 2 * (z - din * mid) + c}

    def real(bb):
        return bb + mir * (3 - 2 * bb)

    barrier = pltpu.get_barrier_semaphore()
    pl.semaphore_signal(barrier, inc=1, device_id=partner, device_id_type=MESH)
    pl.semaphore_signal(barrier, inc=1, device_id=inward, device_id_type=MESH)

    @pl.when(is_mid)
    def _():
        pl.semaphore_signal(barrier, inc=1, device_id=outward, device_id_type=MESH)

    def gu_copy(ref, u, slot, h):
        return pltpu.make_async_copy(
            ref.at[pl.ds(pl.multiple_of((u // NG) * KC, KC), KC),
                   pl.ds(pl.multiple_of((u % NG) * GW, GW), GW)],
            ring.at[slot, :, pl.ds(h * GW, GW)], wsem.at[slot, h])

    def fetch_gu(u, slot):
        gu_copy(wg_ref, u, slot, 0).start()
        gu_copy(wu_ref, u, slot, 1).start()

    def d_copy(d, slot):
        return pltpu.make_async_copy(
            wd_ref.at[pl.ds(pl.multiple_of((d % 2) * FH, FH), FH),
                      pl.ds(pl.multiple_of((d // 2) * 2 * DW, 2 * DW), 2 * DW)],
            ring.at[slot, pl.ds(0, FH)], wsem.at[slot, 0])

    def fetch_d(d):
        d_copy(d, lax.rem(d, NS)).start()

    for u in range(NS - 1):
        fetch_gu(u, u)

    def send_x(src, b, p, sem, recv, dev):
        return pltpu.make_async_remote_copy(
            src_ref=src, dst_ref=xg.at[b, c, p], send_sem=sem.at[b, p],
            recv_sem=recv.at[b, p], device_id=dev, device_id_type=MESH)

    def own_cols(p):
        return x_ref.at[:, pl.ds(pl.multiple_of(p * KC, KC), KC)]

    def own_x(p, kind):
        if kind == 0:
            return send_x(own_cols(p), z, p, d2d_send, agp_recv, partner)
        if kind == 1:
            return send_x(own_cols(p), z, p, fwd_send, ag_recv, inward)
        return send_x(own_cols(p), z, p, out_send, ag_recv, outward)

    def arrived(b, p):
        with jax.named_scope("w_ag"):
            send_x(xg.at[b, c, p], b, p, fwd_send, ag_recv, partner).wait_recv()

    def forward(b, p, dev):
        return send_x(xg.at[b, c, p], b, p, fwd_send, ag_recv, dev)

    def share(b, p):
        return send_x(xg.at[b, c, p], b, p, d2d_send, agp_recv, partner)

    def load_own(b, p):
        return pltpu.make_async_copy(xg.at[b, c, p], xb.at[p, pl.ds(0, R)], xsem.at[0, p])

    def load_partner(b, p):
        return pltpu.make_async_copy(xg.at[b, 1 - c, p], xb.at[p, pl.ds(R, R)], xsem.at[1, p])

    def partner_piece(b, p):
        with jax.named_scope("w_px"):
            pltpu.make_async_remote_copy(
                src_ref=xg.at[b, 1 - c, p], dst_ref=xg.at[b, 1 - c, p],
                send_sem=d2d_send.at[b, p], recv_sem=agp_recv.at[b, p],
                device_id=partner, device_id_type=MESH).wait_recv()
        load_partner(b, p).start()

    def relay_first(p):
        b = real(1 - mid)
        arrived(b, p)

        @pl.when(is_mid)
        def _():
            forward(b, p, inward).start()

        share(b, p).start()
        load_own(b, p).start()

    def partner_first(p):
        partner_piece(real(1 - mid), p)

    def relay_end(s, p):
        arrived(real(5 - s), p)
        share(real(5 - s), p).start()
        load_own(real(5 - s), p).start()

    def partner_end(s, p):
        partner_piece(real(5 - s), p)

    def relay_mid(bb, p):
        arrived(real(bb), p)
        forward(real(bb), p, outward).start()
        share(real(bb), p).start()

    def load_mid(bb):
        @pl.loop(0, NP)
        def _(p):
            load_own(real(bb), p).start()
            partner_piece(real(bb), p)

    def send_pt(s, j):
        k = (ND * (s - 1) + j) % PS
        return pltpu.make_async_remote_copy(
            src_ref=pst.at[k], dst_ref=pt.at[k], send_sem=pst_send.at[k],
            recv_sem=pt_recv.at[k], device_id=partner, device_id_type=MESH)

    def cols_of(k):
        return pl.ds(pl.multiple_of(k * DW, DW), DW)

    def send_rs(slot, there, j, dev):
        sem = 4 if isinstance(there, int) and there == 1 else there
        return pltpu.make_async_remote_copy(
            src_ref=rs.at[slot, j], dst_ref=rs.at[there, j], send_sem=rs_send.at[slot, j],
            recv_sem=rs_recv.at[sem, j], device_id=dev, device_id_type=MESH)

    def send_first(j):
        return pltpu.make_async_remote_copy(
            src_ref=y_ref.at[:, cols_of(j)], dst_ref=y_ref.at[:, cols_of(j)],
            send_sem=rs_send.at[1, j], recv_sem=rs_recv.at[1, j],
            device_id=inward, device_id_type=MESH)

    def rs_arrived(slot, j):
        with jax.named_scope(f"w_rs{slot}"):
            send_rs(0, slot, j, inward).wait_recv()

    def fold(s, k):
        with jax.named_scope("w_pt"):
            send_pt(s, k).wait_recv()
        v = stash[s % 4, k] + pt[(ND * (s - 1) + k) % PS].astype(F32)

        @pl.when(is_end & (s == 1))
        def _():
            y_ref[:, cols_of(k)] = v.astype(BF16)

        @pl.when(is_end & (s > 1) & (s < 4))
        def _():
            rs[s, k] = v.astype(BF16)

        @pl.when(is_mid | (s == 4))
        def _():
            stash[s % 4, k] = v

    def end_send(s, k):
        @pl.when(is_end & (s == 1))
        def _():
            send_first(k).start()

        @pl.when(is_end & (s > 1) & (s < 4))
        def _():
            send_rs(s, s, k, inward).start()

    def add_in(slot, s, k):
        rs_arrived(slot, k)
        rs[slot, k] = (stash[s, k] + rs[slot, k].astype(F32)).astype(BF16)

    def pass_on(k):
        @pl.when(k < ND)
        def _():
            send_rs(2, 0, k, inward).start()

        @pl.when(k >= ND)
        def _():
            send_rs(3, 1, k - ND, inward).start()

    def take(k):
        @pl.when(k < ND)
        def _():
            add_in(2, 2, k)

        @pl.when(k >= ND)
        def _():
            add_in(3, 3, k - ND)

    def x_own(p):
        return pltpu.make_async_copy(own_cols(p), xb.at[p, pl.ds(0, R)], xsem.at[0, p])

    for p in range(NP):
        x_own(p).start()
    with jax.named_scope("w_bar"):
        pl.semaphore_wait(barrier, 2 + mid)

    @pl.loop(0, NP)
    def _(p):
        own_x(p, 0).start()

        @pl.when(is_end | (p == 0))
        def _():
            own_x(p, 1).start()

        @pl.when(is_mid)
        def _():
            own_x(p, 2).start()

    partner_piece(z, 0)

    def gu_events(s, kc, n):
        def at(when, q, fn):
            if q // NG == kc:
                @pl.when(when & (n == q % NG))
                def _():
                    fn()

        first, second, both = s == 0, s == 1, (s == 2) | (s == 3)
        for p in range(1, NP):
            at(first, p - 1, functools.partial(partner_piece, z, p))
        at(first, 9, lambda: relay_first(0))
        at(first, 11, lambda: partner_first(0))
        at(first, 18, lambda: relay_first(1))
        at(first, 19, lambda: partner_first(1))
        at(first & is_mid, 19, lambda: relay_mid(3, 0))
        at(second, 5, lambda: relay_first(2))
        at(second, 7, lambda: partner_first(2))
        at(second & is_mid, 10, lambda: relay_mid(3, 1))
        at(second, 12, lambda: relay_first(3))

        def own_rest():
            for p in range(1, NP):
                own_x(p, 1).start()

        at(second & is_mid, 12, own_rest)
        at(second, 13, lambda: partner_first(3))
        at(second & is_mid, 18, lambda: relay_mid(3, 2))
        for i, q in enumerate((0, 7, 15)):
            at((s == 2) & is_mid, q, functools.partial(relay_mid, 2, 1 + i))
        at(both & is_end, 1, lambda: partner_end(s, 1))
        at(both & is_end, 6, lambda: relay_end(s, 2))
        at(both & is_end, 8, lambda: partner_end(s, 2))
        at(both & is_end, 12, lambda: relay_end(s, 3))
        at(both & is_end, 13, lambda: partner_end(s, 3))
        for i, q in enumerate(TAKES):
            at((s == 3) & is_mid, q, functools.partial(take, jnp.int32(3 + i)))

    def gu_sends(s, kc, n):
        for i, q in enumerate(TAKES):
            if (q + 1) // NG == kc:
                @pl.when((s == 3) & is_mid & (n == (q + 1) % NG))
                def _():
                    pass_on(jnp.int32(3 + i))

    @pl.loop(0, 5)
    def _(s):
        @pl.when(s < 4)
        def _():
            @pl.when(s >= 2)
            def _():
                fetch_gu(2, 2)
                fetch_gu(3, 3)

            for kc in range(NP):
                with jax.named_scope("w_xl"):
                    load_own(z, kc).wait()
                    load_partner(z, kc).wait()

                @pl.loop(0, NG)
                def _(n):
                    if kc < NP - 1:
                        fetch_gu(kc * NG + n + NS - 1, (n + NS - 1) % NS)
                    else:
                        @pl.when(n == 0)
                        def _():
                            fetch_gu(GU - 1, NS - 1)

                        @pl.when((n > 0) & (s == 0))
                        def _():
                            fetch_gu(n - 1, n - 1)

                        @pl.when((n > 0) & (s > 0))
                        def _():
                            fetch_d(n - 1)

                    gu_sends(s, kc, n)
                    with jax.named_scope("w_wg"):
                        gu_copy(wg_ref, kc * NG + n, n, 0).wait()
                        gu_copy(wu_ref, kc * NG + n, n, 1).wait()
                    with jax.named_scope("gu"):
                        t = jnp.dot(xb[kc], ring[n], preferred_element_type=F32)
                        if kc == 0:
                            acc[n] = t
                        elif kc < NP - 1:
                            acc[n] += t
                        else:
                            t += acc[n]
                            hid[(s + 3) // 4, :, pl.ds(pl.multiple_of(n * GW, GW), GW)] = (
                                jax.nn.silu(t[:, :GW]) * t[:, GW:]).astype(BF16)
                    gu_events(s, kc, n)

        @pl.when(s > 0)
        def _():
            @pl.when(is_mid & (s >= 3))
            def _():
                take(12 + 5 * (s - 3))

            @pl.loop(0, ND2)
            def _(j):
                s0, s1 = lax.rem(2 * j, NS), lax.rem(2 * j + 1, NS)

                @pl.when(j == 0)
                def _():
                    @pl.when(s == 4)
                    def _():
                        fetch_d(jnp.int32(2))
                        fetch_d(jnp.int32(3))

                    fetch_d(jnp.int32(4))

                @pl.when((j > 0) & (j < 6))
                def _():
                    fetch_d(2 * j + 3)

                @pl.when((j > 0) & (j < 5))
                def _():
                    fetch_d(2 * j + 4)

                @pl.when((j == 6) & (s < 3))
                def _():
                    fetch_gu(0, 0)
                    fetch_gu(1, 1)

                @pl.when((j == 6) & (s == 3))
                def _():
                    fetch_d(jnp.int32(0))
                    fetch_d(jnp.int32(1))

                @pl.when(is_mid & (s >= 3) & (j == 0))
                def _():
                    pass_on(12 + 5 * (s - 3))

                with jax.named_scope("w_wd"):
                    d_copy(2 * j, s0).wait()
                    d_copy(2 * j + 1, s1).wait()

                @pl.when(j >= 2)
                def _():
                    for h in range(2):
                        send_pt(s, 2 * j - PS + h).wait_send()

                hs = 1 - s // 4
                for h in range(2):
                    with jax.named_scope("d"):
                        cols = slice(h * DW, (h + 1) * DW)
                        t = jnp.dot(hid[hs, :, :FH], ring[s0, :FH, cols],
                                    preferred_element_type=F32)
                        t += jnp.dot(hid[hs, :, FH:], ring[s1, :FH, cols],
                                     preferred_element_type=F32)
                        stash[s % 4, 2 * j + h] = t[:R]
                        pst[(ND * (s - 1) + 2 * j + h) % PS] = t[R:].astype(BF16)

                def for_middle(do):
                    @pl.when((s == 2) & (j >= 3) & (j < 6))
                    def _():
                        do(j - 3)

                    @pl.when((s == 3) & (j % 3 != 2) & (j > 0))
                    def _():
                        do(12 + j - j // 3)

                    @pl.when((s == 4) & (j % 3 != 0))
                    def _():
                        do(17 + j - j // 3)

                def for_outer(do):
                    @pl.when(is_mid & (s >= 3))
                    def _():
                        do((s - 3) * ND2 + j)

                @pl.when(is_mid)
                def _():
                    for_middle(take)

                for_outer(lambda k: add_in(0, 1, k))

                @pl.when(j >= 1)
                def _():
                    fold(s, 2 * j - 2)
                    fold(s, 2 * j - 1)

                for h in range(2):
                    send_pt(s, 2 * j + h).start()

                @pl.when(j >= 1)
                def _():
                    end_send(s, 2 * j - 2)
                    end_send(s, 2 * j - 1)

                @pl.when(is_mid)
                def _():
                    for_middle(pass_on)

                for_outer(lambda k: send_rs(0, 0, k, outward).start())

                @pl.when((s == 1) | (s == 2))
                def _():
                    @pl.when(is_end & ((j == 0) | (j == 6)))
                    def _():
                        relay_end(s + 1, j // 6)

                    @pl.when(is_end & (j == 1))
                    def _():
                        partner_end(s + 1, 0)

                    @pl.when(is_mid & (s == 1) & (j == 3))
                    def _():
                        relay_mid(3, 3)
                        relay_mid(2, 0)

                    @pl.when(is_mid & (j == 5))
                    def _():
                        load_mid(4 - s)

            fold(s, ND - 2)
            fold(s, ND - 1)

            @pl.loop(ND - PS, ND)
            def _(k):
                send_pt(s, k).wait_send()

            end_send(s, ND - 2)
            end_send(s, ND - 1)

    @pl.loop(0, NP)
    def _(p):
        own_x(p, 0).wait_send()
        own_x(p, 1).wait_send()

        @pl.when(is_mid)
        def _():
            own_x(p, 2).wait_send()
            for bb in (0, 2, 3):
                forward(real(bb), p, inward).wait_send()
                share(real(bb), p).wait_send()

        @pl.when(is_end)
        def _():
            for bb in (1, 2, 3):
                share(real(bb), p).wait_send()

    @pl.when(is_mid)
    def _():
        def finish(k):
            send_first(k).wait_recv()
            rs_arrived(1, k)
            y_ref[:, cols_of(k)] = (
                stash[0, k] + y_ref[:, cols_of(k)].astype(F32) + rs[1, k].astype(F32)).astype(BF16)

        def done(k):
            send_rs(2, 0, k, inward).wait_send()
            send_rs(0, 0, k, outward).wait_send()
            send_rs(3, 1, k, inward).wait_send()

        @pl.loop(0, ND2)
        def _(i):
            @pl.when(i < ND2 - 1)
            def _():
                add_in(3, 3, 8 + i)

            finish(2 * i)

            @pl.when(i < ND2 - 1)
            def _():
                send_rs(3, 1, 8 + i, inward).start()

            finish(2 * i + 1)

            @pl.when(i > 0)
            def _():
                done(2 * i - 2)
                done(2 * i - 1)

        done(ND - 2)
        done(ND - 1)

    @pl.when(is_end)
    def _():
        @pl.loop(0, ND)
        def _(k):
            rs_arrived(0, k)
            send_first(k).wait_send()
            y_ref[:, cols_of(k)] = (stash[0, k] + rs[0, k].astype(F32)).astype(BF16)
            for s in (2, 3):
                send_rs(s, s, k, inward).wait_send()


def solution(mesh):
    dma = pltpu.SemaphoreType.DMA

    def step(x, w_gate, w_up, w_down):
        hbm = pl.BlockSpec(memory_space=pltpu.HBM)
        y, _ = pl.pallas_call(
            kernel,
            name="mlp",
            out_shape=(pltpu.VMEM((R, D), BF16),
                       jax.ShapeDtypeStruct((4, 2, NP, R, KC), BF16)),
            in_specs=[hbm] * 4,
            out_specs=(pl.BlockSpec(memory_space=pltpu.VMEM), hbm),
            scratch_shapes=[
                pltpu.VMEM((NP, 2 * R, KC), BF16),
                pltpu.VMEM((NS, KC, 2 * GW), BF16),
                pltpu.VMEM((2, 2 * R, F), BF16),
                pltpu.VMEM((NG, 2 * R, 2 * GW), F32),
                pltpu.VMEM((4, ND, R, DW), F32),
                pltpu.VMEM((PS, R, DW), BF16),
                pltpu.VMEM((PS, R, DW), BF16),
                pltpu.VMEM((4, ND, R, DW), BF16),
                dma((NS, 2)), dma((2, NP)),
                dma((4, NP)), dma((4, NP)), dma((4, NP)), dma((4, NP)), dma((4, NP)),
                dma((PS,)), dma((PS,)), dma((4, ND)), dma((5, ND)),
            ],
            compiler_params=pltpu.CompilerParams(
                collective_id=0, has_side_effects=True, vmem_limit_bytes=64600000),
        )(x, w_gate, w_up, w_down)
        return y

    return jax.shard_map(
        step,
        mesh=mesh,
        in_specs=(P(("dp", "tp"), None), P(None, "tp"), P(None, "tp"), P("tp", None)),
        out_specs=P(("dp", "tp"), None),
        check_vma=False,
    )
```
